128 devices in a mesh: sub: 4 (over x_hi, core), brick: 32 (over x_lo, z, y).
Axes of the slice: x: 4 (x_hi: 2, x_lo: 2; x = x_hi * 2 + x_lo), y: 4, z: 4, core: 2. Of those that a mesh axis runs over, the one named last changes fastest.
Arguments:
- increments: float32 [8, 128, 256, 512], P('sub', None, 'brick'), may hold values from -6 to 6
- courant_x: float32 [8, 128, 256, 512], P('sub', None, 'brick'), may hold values from -0.5 to 0.5
- courant_y: float32 [8, 128, 256, 512], P('sub', None, 'brick'), may hold values from -0.5 to 0.5
- spectrum: float32 [256, 512], replicated, may hold values from 0.05 to 2
- vertical: float32 [128, 128], replicated, may hold values from -0.5 to 0.5
Outputs:
- covaried: float32 [8, 128, 256, 512], P('sub', None, 'brick')
The draws below stay inside these ranges and needn't reach their ends.
All inputs are finite; a program needn't handle non-finite values.
Results may differ from the reference program's by a relative error of at most 0.00007.
Values sent between devices are 32-bit elements; how exact they have to be, the bound alone decides.
A program may use at most 192 MiB of HBM per device.

```python
import math
import jax
import jax.numpy as jnp
from jax import lax

NX = 256
NY = 512
L = 128
STEPS = 4
SUBS = 8


def levels(own_key, dims, shards, least, largest):
    level = 1.0
    for position, parts in shards:
        heights = jax.random.uniform(jax.random.fold_in(jax.random.fold_in(own_key, 6), position), (parts,), jnp.float32, least / len(shards), largest / len(shards))
        level = level * jnp.repeat(jnp.exp(heights), dims[position] // parts).reshape((-1,) + (1,) * (len(dims) - 1 - position))
    return level


def noise(rng, dims, spread, bound, pieces=(), kind=jnp.bfloat16):
    array = jax.random.normal(rng, dims, jnp.float32) * spread
    if len(pieces) > 0:
        array = levels(rng, dims, pieces, -0.22, 0.18) * array
    return jnp.clip(array, min=-bound, max=bound).astype(kind)


def setup_inputs(seed: int = 0) -> dict:
    streams_of = jax.random.split(jax.random.key(seed), 6)
    increments = noise(streams_of[0], (SUBS, L, NX, NY), 1.0, 6.0, ((0, 4), (2, 32)), jnp.float32)
    courant_x = jnp.clip(jax.random.uniform(streams_of[1], (SUBS, L, NX, NY), jnp.float32, -0.5, 0.5) * levels(streams_of[1], (SUBS, L, NX, NY), ((0, 4), (2, 32)), -0.4, 0.0), -0.5, 0.5)
    courant_y = jnp.clip(jax.random.uniform(streams_of[2], (SUBS, L, NX, NY), jnp.float32, -0.5, 0.5) * levels(streams_of[2], (SUBS, L, NX, NY), ((0, 4), (2, 32)), -0.4, 0.0), -0.5, 0.5)
    spectrum = jnp.clip(jnp.exp(jax.random.uniform(streams_of[3], (NX, NY), jnp.float32, math.log(0.05), math.log(2.0))), 0.05, 2.0)
    vertical = noise(streams_of[4], (L, L), L ** -0.5, 0.5, (), jnp.float32)
    return dict(increments=increments, courant_x=courant_x, courant_y=courant_y, spectrum=spectrum, vertical=vertical)


diffusion = 0.2

def dct_table(count):
    freq = jnp.arange(count, dtype=jnp.float32)[:, None]
    cells = jnp.arange(count, dtype=jnp.float32)[None, :]
    table = jnp.cos(jnp.pi * (cells + 0.5) * freq / count) * jnp.sqrt(jnp.float32(2.0) / count)
    first = jnp.where(jnp.arange(count)[:, None] == 0, jnp.sqrt(jnp.float32(0.5)), jnp.float32(1.0))
    return table * first

def advance(extended, courant_x, courant_y):
    center = extended[..., 1:-1, :]
    north = extended[..., 2:, :]
    south = extended[..., :-2, :]
    widths = [(0, 0)] * (center.ndim - 1) + [(1, 1)]
    padded = jnp.pad(center, widths)
    east = padded[..., 2:]
    west = padded[..., :-2]
    return center - 0.5 * courant_x * (north - south) - 0.5 * courant_y * (east - west) + diffusion * (north + south + east + west - 4.0 * center)

def propagate(triple):
    state, speed_x, speed_y = triple
    for number in range(STEPS):
        extended = jnp.pad(state, ((0, 0), (1, 1), (0, 0)))
        state = advance(extended, speed_x, speed_y)
    return state

def reference(increments, courant_x, courant_y, spectrum, vertical):
    ends = lax.map(propagate, (increments, courant_x, courant_y))
    previous = jnp.concatenate([jnp.zeros_like(ends[:1]), ends[:-1]], axis=0)
    jumps = increments - previous
    row_table = dct_table(NX)
    col_table = dct_table(NY)
    high = lax.Precision.HIGHEST

    def covary(block):
        forward = jnp.einsum('kx,lxy->lky', row_table, block, precision=high)
        forward = jnp.einsum('lky,jy->lkj', forward, col_table, precision=high)
        scaled = forward * spectrum
        back = jnp.einsum('lkj,jy->lky', scaled, col_table, precision=high)
        back = jnp.einsum('kx,lky->lxy', row_table, back, precision=high)
        return jnp.einsum('ml,lxy->mxy', vertical, back, precision=high)
    return lax.map(covary, jumps)
```

```python
import jax
import jax.numpy as jnp
import ml_dtypes
import numpy as np
from jax import lax
from jax.experimental import pallas as pl
from jax.experimental.pallas import tpu as pltpu
from jax.sharding import PartitionSpec as P

STEPS = 4
ROWS, LEVELS, COLS, NX = 8, 128, 512, 256
MESH = pl.DeviceIdType.MESH
F32, BF16 = jnp.float32, jnp.bfloat16
EVEN, ODD_A, ODD_B = (0, 0, 128), (1, 0, 64), (1, 64, 64)
STREAMS = (EVEN, ODD_A, ODD_B)
XZ_ORDER = ((1, 0), (0, 1), (1, 1), (0, 3), (1, 3), (0, 2), (1, 2))


def dct_table(count):
    one = np.float32
    freq = np.arange(count, dtype=one)[:, None]
    cells = np.arange(count, dtype=one)[None, :]
    angle = one(np.pi) * (cells + one(0.5)) * freq / one(count)
    table = np.cos(angle.astype(np.float64)).astype(one) * np.sqrt(one(2.0) / one(count))
    table[0] *= np.sqrt(one(0.5))
    return table


def halves(table):
    high = table.astype(ml_dtypes.bfloat16)
    low = (table - high.astype(np.float32)).astype(ml_dtypes.bfloat16)
    return np.stack([high, low])


def split(value):
    high = value.astype(BF16)
    return high, (value - high.astype(F32)).astype(BF16)


def product(a, b):
    def dot(u, v):
        return jnp.dot(u, v, preferred_element_type=F32)

    return dot(a[0], b[0]) + (dot(a[0], b[1]) + dot(a[1], b[0]))


def kernel(
    inc_hbm, cx_hbm, cy_hbm, spec_hbm, vert_hbm, rt_hbm, rtt_hbm, ct_hbm, ctt_hbm,
    out_hbm,
    inc, cx, cy, one_buf, two_buf, halo, prior, jumps, mid, planes, mid_back, done,
    spec, vert, rt, rtt, ct, ctt,
    load_sem, table_sem, halo_send, halo_recv, prior_send, prior_recv,
    a_send, a_recv, b_send, b_recv, c_send, c_recv, d_send, d_recv, out_sem,
):
    sub, brick = lax.axis_index("sub"), lax.axis_index("brick")
    x, z, y = brick // 16, lax.rem(brick // 4, 4), lax.rem(brick, 4)
    mine = x * 4 + z
    up, down = lax.rem(brick + 1, 32), lax.rem(brick + 31, 32)
    keep_up = jnp.where(brick == 31, 0.0, 1.0).astype(F32)
    keep_down = jnp.where(brick == 0, 0.0, 1.0).astype(F32)

    def xz_peer(dx, dz):
        px, pz = lax.rem(x + dx, 2), lax.rem(z + dz, 4)
        return px * 4 + pz, {"brick": px * 16 + pz * 4 + y}

    def y_peer(dy):
        py = lax.rem(y + dy, 4)
        return py, {"brick": brick - y + py}

    def remote(src, dst, send, recv, device):
        return pltpu.make_async_remote_copy(
            src_ref=src, dst_ref=dst, send_sem=send, recv_sem=recv, device_id=device, device_id_type=MESH
        )

    loads = {}

    def load(name, src, dst, s, rows):
        for r in rows:
            copy = pltpu.make_async_copy(src.at[s, :, r, :], dst.at[s, r], load_sem.at[len(loads)])
            copy.start()
            loads[name, s, r] = copy

    edges, inner = (0, 7), tuple(range(1, 7))
    for s in (0, 1):
        load("inc", inc_hbm, inc, s, edges)
    load("inc", inc_hbm, inc, 0, inner)
    load("cx", cx_hbm, cx, 0, edges + inner)
    load("cy", cy_hbm, cy, 0, edges + inner)
    load("inc", inc_hbm, inc, 1, inner)
    load("cx", cx_hbm, cx, 1, edges + inner)
    load("cy", cy_hbm, cy, 1, edges + inner)
    tables = [
        pltpu.make_async_copy(src, dst, table_sem.at[i])
        for i, (src, dst) in enumerate(
            ((vert_hbm, vert), (spec_hbm, spec), (rt_hbm, rt), (rtt_hbm, rtt), (ct_hbm, ct), (ctt_hbm, ctt))
        )
    ]
    for copy in tables:
        copy.start()

    barrier = pltpu.get_barrier_semaphore()
    peers = [{"brick": up}, {"brick": down}, {"sub": lax.rem(sub + 1, 4)}, {"sub": lax.rem(sub + 3, 4)}]
    peers += [xz_peer(dx, dz)[1] for dx, dz in XZ_ORDER] + [y_peer(dy)[1] for dy in (1, 2, 3)]
    for peer in peers:
        pl.semaphore_signal(barrier, inc=1, device_id=peer, device_id_type=MESH)

    pl.semaphore_wait(barrier, len(peers))

    def state(step):
        return inc if step == 0 else (one_buf if step % 2 else two_buf)

    def halo_copies(stream, step):
        s, low, count = stream
        n, t = STREAMS.index(stream), step - 1
        levels = pl.ds(low, count)
        src = state(step - 1)
        return (
            remote(src.at[s, 7, levels], halo.at[s, t, 0, levels], halo_send.at[n, t, 0], halo_recv.at[n, t, 0], {"brick": up}),
            remote(src.at[s, 0, levels], halo.at[s, t, 1, levels], halo_send.at[n, t, 1], halo_recv.at[n, t, 1], {"brick": down}),
        )

    def rows(stream, step, which, block):
        s, low, count = stream
        src, dst = state(step - 1), state(step)
        lane = lax.broadcasted_iota(jnp.int32, (block, COLS), 1)

        def body(i, carry):
            at = pl.ds(pl.multiple_of(low + i * block, 8), block)
            for r in which:
                center = src[s, r, at]
                north = src[s, r + 1, at] if r < 7 else halo[s, step - 1, 1, at] * keep_up
                south = src[s, r - 1, at] if r > 0 else halo[s, step - 1, 0, at] * keep_down
                east = jnp.where(lane == COLS - 1, 0.0, pltpu.roll(center, COLS - 1, 1))
                west = jnp.where(lane == 0, 0.0, pltpu.roll(center, 1, 1))
                flow = cx[s, r, at] * (north - south) + cy[s, r, at] * (east - west)
                spread = (north + south) + (east + west) - 4.0 * center
                dst[s, r, at] = center - 0.5 * flow + 0.2 * spread
            return carry

        lax.fori_loop(0, count // block, body, 0)

    def event(stream, step):
        s, low, count = stream
        for copy in halo_copies(stream, step):
            copy.wait_recv()
        if step >= 3:
            for copy in halo_copies(stream, step - 1):
                copy.wait_send()
        rows(stream, step, edges, 16)
        if step < STEPS:
            for copy in halo_copies(stream, step + 1):
                copy.start()
        rows(stream, step, inner, 8)

    def start_chunks(s, ends, first):
        weights = split(vert[...])
        for r in range(ROWS):
            mixed = product(weights, split(inc[s, r] - ends[r]))
            for c in range(4):
                jumps[first + c, :, r, :] = mixed[32 * c : 32 * c + 32]
        for c in range(4):
            k = first + c
            for dx, dz in XZ_ORDER:
                there, device = xz_peer(dx, dz)
                remote(jumps.at[k, pl.ds(there * 4, 4)], mid.at[k, mine], a_send.at[k], a_recv.at[k], device).start()

    def a_all(k):
        part = mid.at[k, pl.ds(0, 7)]
        return remote(part, part, a_send.at[k], a_recv.at[k], {"brick": up})

    def b_all(k):
        return remote(planes.at[k, pl.ds(0, 6)], planes.at[k, pl.ds(0, 6)], b_send.at[k], b_recv.at[k], {"brick": up})

    def c_all(k):
        return remote(mid_back.at[k, pl.ds(0, 6)], mid_back.at[k, pl.ds(0, 6)], c_send.at[k], c_recv.at[k], {"brick": up})

    def d_all(k):
        return remote(done.at[k, pl.ds(0, 28)], done.at[k, pl.ds(0, 28)], d_send.at[k], d_recv.at[k], {"brick": up})

    def second_hop(k):
        a_all(k).wait_recv()
        mid[k, mine] = jumps[k, pl.ds(mine * 4, 4)]
        for dy in (1, 3, 2):
            there, device = y_peer(dy)
            remote(mid.at[k, :, there], planes.at[k, :, y], b_send.at[k], b_recv.at[k], device).start()
        planes[k, :, y] = mid[k, :, y]

    def transform(k):
        b_all(k).wait_recv()
        plane = planes[k].reshape(NX, COLS)
        value = product((rt[0], rt[1]), split(plane))
        value = product(split(value), (ctt[0], ctt[1])) * spec[...]
        value = product(split(value), (ct[0], ct[1]))
        value = product((rtt[0], rtt[1]), split(value))
        planes[k] = value.reshape(8, 4, ROWS, COLS)
        for dy in (1, 3, 2):
            there, device = y_peer(dy)
            remote(planes.at[k, :, there], mid_back.at[k, :, y], c_send.at[k], c_recv.at[k], device).start()
        mid_back[k, :, y] = planes[k, :, y]

    def fourth_hop(k):
        c_all(k).wait_recv()
        for dx, dz in XZ_ORDER:
            there, device = xz_peer(dx, dz)
            remote(mid_back.at[k, there], done.at[k, pl.ds(mine * 4, 4)], d_send.at[k], d_recv.at[k], device).start()
        done[k, pl.ds(mine * 4, 4)] = mid_back[k, mine]

    def out_copy(k):
        s, c = (1, k) if k < 4 else (0, k - 4)
        return pltpu.make_async_copy(done.at[k], out_hbm.at[s, pl.ds(32 * c, 32)], out_sem.at[k])

    def finish(k):
        d_all(k).wait_recv()
        out_copy(k).start()

    for s in (0, 1):
        for r in edges:
            loads["inc", s, r].wait()
        for stream in STREAMS:
            if stream[0] == s:
                for copy in halo_copies(stream, 1):
                    copy.start()
    for s in (0, 1):
        for r in inner:
            loads["inc", s, r].wait()
        for r in range(ROWS):
            loads["cx", s, r].wait()
            loads["cy", s, r].wait()
        if s == 0:
            event(EVEN, 1)
    event(ODD_A, 1)
    event(EVEN, 2)
    event(ODD_B, 1)
    event(EVEN, 3)
    event(ODD_A, 2)
    event(EVEN, 4)
    event(ODD_B, 2)
    tables[0].wait()
    start_chunks(1, two_buf.at[0], 0)
    event(ODD_A, 3)
    event(ODD_B, 3)

    def prior_copy(stream):
        s, low, count = stream
        n = STREAMS.index(stream) - 1
        levels = pl.ds(low, count)
        return remote(
            two_buf.at[1, :, levels], prior.at[:, levels], prior_send.at[n], prior_recv.at[n], {"sub": lax.rem(sub + 1, 4)}
        )

    for stream in (ODD_A, ODD_B):
        event(stream, 4)

        @pl.when(sub < 3)
        def _():
            prior_copy(stream).start()

    @pl.when(sub == 0)
    def _():
        prior[...] = jnp.zeros(prior.shape, F32)

    for copy in tables[1:]:
        copy.wait()
    for k in range(4):
        second_hop(k)

    def odd_planes(k, carry):
        transform(k)
        return carry

    lax.fori_loop(0, 4, odd_planes, 0)

    @pl.when(sub > 0)
    def _():
        for stream in (ODD_A, ODD_B):
            prior_copy(stream).wait_recv()

    start_chunks(0, prior, 4)
    for k in range(4):
        fourth_hop(k)
        second_hop(k + 4)

    def even_planes(k, carry):
        transform(k)
        return carry

    lax.fori_loop(4, 8, even_planes, 0)
    for k in range(4):
        finish(k)
    for k in range(4, 8):
        fourth_hop(k)
    for k in range(4, 8):
        finish(k)

    for stream in STREAMS:
        for step in (1, STEPS):
            for copy in halo_copies(stream, step):
                copy.wait_send()

    @pl.when(sub < 3)
    def _():
        for stream in (ODD_A, ODD_B):
            prior_copy(stream).wait_send()

    for k in range(8):
        a_all(k).wait_send()
        b_all(k).wait_send()
        c_all(k).wait_send()
        d_all(k).wait_send()
        out_copy(k).wait()


def on_device(increments, courant_x, courant_y, spectrum, vertical):
    row_table, col_table = dct_table(NX), dct_table(COLS)
    tables = [halves(t) for t in (row_table, row_table.T, col_table, col_table.T)]
    hbm = pl.BlockSpec(memory_space=pl.ANY)
    slabs = (2, ROWS, LEVELS, COLS)
    dma = pltpu.SemaphoreType.DMA
    return pl.pallas_call(
        kernel,
        out_shape=jax.ShapeDtypeStruct((2, LEVELS, ROWS, COLS), F32),
        in_specs=[hbm] * 9,
        out_specs=hbm,
        scratch_shapes=[
            pltpu.VMEM(slabs, F32),
            pltpu.VMEM(slabs, F32),
            pltpu.VMEM(slabs, F32),
            pltpu.VMEM(slabs, F32),
            pltpu.VMEM(slabs, F32),
            pltpu.VMEM((2, STEPS, 2, LEVELS, COLS), F32),
            pltpu.VMEM((ROWS, LEVELS, COLS), F32),
            pltpu.VMEM((8, 32, ROWS, COLS), F32),
            pltpu.VMEM((8, 8, 4, ROWS, COLS), F32),
            pltpu.VMEM((8, 8, 4, ROWS, COLS), F32),
            pltpu.VMEM((8, 8, 4, ROWS, COLS), F32),
            pltpu.VMEM((8, 32, ROWS, COLS), F32),
            pltpu.VMEM((NX, COLS), F32),
            pltpu.VMEM((LEVELS, LEVELS), F32),
            pltpu.VMEM((2, NX, NX), BF16),
            pltpu.VMEM((2, NX, NX), BF16),
            pltpu.VMEM((2, COLS, COLS), BF16),
            pltpu.VMEM((2, COLS, COLS), BF16),
            dma((48,)),
            dma((6,)),
            dma((3, STEPS, 2)),
            dma((3, STEPS, 2)),
            dma((2,)),
            dma((2,)),
            *[dma((8,)) for _ in range(9)],
        ],
        compiler_params=pltpu.CompilerParams(
            collective_id=0, has_side_effects=True, vmem_limit_bytes=67_043_328
        ),
    )(increments, courant_x, courant_y, spectrum, vertical, *[jnp.asarray(t) for t in tables])


def solution(mesh):
    wide = P("sub", None, "brick", None)
    return jax.shard_map(
        on_device, mesh=mesh, in_specs=(wide, wide, wide, P(), P()), out_specs=wide, check_vma=False
    )
```

```python
import jax
import jax.numpy as jnp
import ml_dtypes
import numpy as np
from jax import lax
from jax.experimental import pallas as pl
from jax.experimental.pallas import tpu as pltpu
from jax.sharding import PartitionSpec as P

STEPS = 4
ROWS, LEVELS, COLS, NX = 8, 128, 512, 256
MESH = pl.DeviceIdType.MESH
F32, BF16 = jnp.float32, jnp.bfloat16
CHUNKS, CHUNK = 8, 32
XZ_ORDER = ((1, 0), (0, 1), (1, 1), (0, 3), (1, 3), (0, 2), (1, 2))


def dct_table(count):
    one = np.float32
    freq = np.arange(count, dtype=one)[:, None]
    cells = np.arange(count, dtype=one)[None, :]
    angle = one(np.pi) * (cells + one(0.5)) * freq / one(count)
    table = np.cos(angle.astype(np.float64)).astype(one) * np.sqrt(one(2.0) / one(count))
    table[0] *= np.sqrt(one(0.5))
    return table


def halves(table):
    high = table.astype(ml_dtypes.bfloat16)
    low = (table - high.astype(np.float32)).astype(ml_dtypes.bfloat16)
    return np.stack([high, low])


def split(value):
    high = value.astype(BF16)
    return high, (value - high.astype(F32)).astype(BF16)


def product(a, b):
    def dot(u, v):
        return jnp.dot(u, v, preferred_element_type=F32)

    return dot(a[0], b[0]) + (dot(a[0], b[1]) + dot(a[1], b[0]))


def kernel(
    inc_hbm, cx_hbm, cy_hbm, spec_hbm, rt_hbm, rtt_hbm, ct_hbm, ctt_hbm,
    out_hbm,
    inc, cx, cy, one_buf, two_buf, halo, prior, jumps, mid, planes, mid_back, done,
    spec, rt, rtt, ct, ctt,
    load_sem, table_sem, halo_send, halo_recv, prior_send, prior_recv,
    a_send, a_recv, b_send, b_recv, c_send, c_recv, d_send, d_recv, out_sem,
):
    sub, brick = lax.axis_index("sub"), lax.axis_index("brick")
    x, z, y = brick // 16, lax.rem(brick // 4, 4), lax.rem(brick, 4)
    mine = x * 4 + z
    up, down = lax.rem(brick + 1, 32), lax.rem(brick + 31, 32)

    def xz_peer(dx, dz):
        px, pz = lax.rem(x + dx, 2), lax.rem(z + dz, 4)
        return px * 4 + pz, {"brick": px * 16 + pz * 4 + y}

    def y_peer(dy):
        py = lax.rem(y + dy, 4)
        return py, {"brick": brick - y + py}

    def remote(src, dst, send, recv, device):
        return pltpu.make_async_remote_copy(
            src_ref=src, dst_ref=dst, send_sem=send, recv_sem=recv, device_id=device, device_id_type=MESH
        )

    loads = []

    def load(src, dst, s, rows):
        for r in rows:
            copy = pltpu.make_async_copy(src.at[s, :, r, :], dst.at[s, r], load_sem.at[len(loads)])
            copy.start()
            loads.append(copy)

    edges, inner = (0, 7), tuple(range(1, 7))
    for s in (1, 0):
        load(inc_hbm, inc, s, edges)
    for s in (1, 0):
        load(inc_hbm, inc, s, inner)
        load(cx_hbm, cx, s, edges + inner)
        load(cy_hbm, cy, s, edges + inner)
    tables = [
        pltpu.make_async_copy(src, dst, table_sem.at[i])
        for i, (src, dst) in enumerate(
            ((spec_hbm, spec), (rt_hbm, rt), (rtt_hbm, rtt), (ct_hbm, ct), (ctt_hbm, ctt))
        )
    ]
    for copy in tables:
        copy.start()

    barrier = pltpu.get_barrier_semaphore()
    peers = [{"brick": up}, {"brick": down}, {"sub": lax.rem(sub + 1, 4)}, {"sub": lax.rem(sub + 3, 4)}]
    peers += [xz_peer(dx, dz)[1] for dx, dz in XZ_ORDER] + [y_peer(dy)[1] for dy in (1, 2, 3)]
    for peer in peers:
        pl.semaphore_signal(barrier, inc=1, device_id=peer, device_id_type=MESH)

    pl.semaphore_wait(barrier, len(peers))

    def state(step):
        return inc if step == 0 else (one_buf if step % 2 else two_buf)

    def place(i):
        return 1 - lax.rem(i, 2), pl.multiple_of((i // 2) * CHUNK, CHUNK)

    def halo_copies(i, step):
        s, low = place(i)
        t, src, levels = step - 1, state(step - 1), pl.ds(low, CHUNK)
        return (
            remote(src.at[s, 7, levels], halo.at[s, t, 0, levels], halo_send.at[i, t, 0], halo_recv.at[i, t, 0], {"brick": up}),
            remote(src.at[s, 0, levels], halo.at[s, t, 1, levels], halo_send.at[i, t, 1], halo_recv.at[i, t, 1], {"brick": down}),
        )

    def halo_do(i, step, verb):
        live = jnp.logical_or(sub < 3, lax.rem(i, 2) == 1)
        upward, downward = halo_copies(i, step)
        below, above = (upward, downward) if verb == "wait_recv" else (downward, upward)
        pl.when(jnp.logical_and(live, brick > 0))(lambda: getattr(below, verb)())
        pl.when(jnp.logical_and(live, brick < 31))(lambda: getattr(above, verb)())

    def rows(i, step, which, block):
        s, low = place(i)
        src, dst = state(step - 1), state(step)
        lane = lax.broadcasted_iota(jnp.int32, (block, COLS), 1)

        def body(n, carry):
            at = pl.ds(pl.multiple_of(low + n * block, 8), block)
            for r in which:
                center = src[s, r, at]
                north = src[s, r + 1, at] if r < 7 else halo[s, step - 1, 1, at]
                south = src[s, r - 1, at] if r > 0 else halo[s, step - 1, 0, at]
                east = jnp.where(lane == COLS - 1, 0.0, pltpu.roll(center, COLS - 1, 1))
                west = jnp.where(lane == 0, 0.0, pltpu.roll(center, 1, 1))
                flow = cx[s, r, at] * (north - south) + cy[s, r, at] * (east - west)
                spread = (north + south) + (east + west) - 4.0 * center
                dst[s, r, at] = center - 0.5 * flow + 0.2 * spread
            return carry

        lax.fori_loop(0, CHUNK // block, body, 0)

    def edge_event(i, step):
        halo_do(i, step, "wait_recv")
        if step >= 3:
            halo_do(i, step - 1, "wait_send")
        rows(i, step, edges, 16)
        if step < STEPS:
            halo_do(i, step + 1, "start")

    def inner_event(i, step):
        rows(i, step, inner, 8)

    def prior_copy(i):
        levels = pl.ds(place(i)[1], CHUNK)
        return remote(
            two_buf.at[1, :, levels], prior.at[:, levels], prior_send.at[i // 2], prior_recv.at[i // 2],
            {"sub": lax.rem(sub + 1, 4)},
        )

    def start_chunk(k, s, ends):
        levels = pl.ds(place(k)[1], CHUNK)
        for r in range(ROWS):
            jumps[k, :, r, :] = inc[s, r, levels] - ends[r, levels]
        for dx, dz in XZ_ORDER:
            there, device = xz_peer(dx, dz)
            remote(jumps.at[k, pl.ds(there * 4, 4)], mid.at[k, mine], a_send.at[k], a_recv.at[k], device).start()

    def a_all(k):
        part = mid.at[k, pl.ds(0, 7)]
        return remote(part, part, a_send.at[k], a_recv.at[k], {"brick": up})

    def b_all(k):
        return remote(planes.at[k, pl.ds(0, 6)], planes.at[k, pl.ds(0, 6)], b_send.at[k], b_recv.at[k], {"brick": up})

    def c_all(k):
        return remote(mid_back.at[k, pl.ds(0, 7)], mid_back.at[k, pl.ds(0, 7)], c_send.at[k], c_recv.at[k], {"brick": up})

    def d_all(k):
        return remote(done.at[k, pl.ds(0, 6)], done.at[k, pl.ds(0, 6)], d_send.at[k], d_recv.at[k], {"brick": up})

    def second_hop(k):
        a_all(k).wait_recv()
        mid[k, mine] = jumps[k, pl.ds(mine * 4, 4)]
        for dy in (1, 3, 2):
            there, device = y_peer(dy)
            remote(mid.at[k, :, there], planes.at[k, :, y], b_send.at[k], b_recv.at[k], device).start()
        planes[k, :, y] = mid[k, :, y]

    def transform(k):
        b_all(k).wait_recv()
        plane = planes[k].reshape(NX, COLS)
        value = product((rt[0], rt[1]), split(plane))
        value = product(split(value), (ctt[0], ctt[1])) * spec[...]
        value = product(split(value), (ct[0], ct[1]))
        value = product((rtt[0], rtt[1]), split(value))
        planes[k] = value.reshape(8, 4, ROWS, COLS)
        for dx, dz in XZ_ORDER:
            there, device = xz_peer(dx, dz)
            remote(planes.at[k, there], mid_back.at[k, mine], c_send.at[k], c_recv.at[k], device).start()
        mid_back[k, mine] = planes[k, mine]

    def fourth_hop(k):
        c_all(k).wait_recv()
        for dy in (1, 3, 2):
            there, device = y_peer(dy)
            remote(mid_back.at[k, :, there], done.at[k, :, y], d_send.at[k], d_recv.at[k], device).start()
        done[k, :, y] = mid_back[k, :, y]

    def out_copy(k):
        return pltpu.make_async_copy(done.at[k], out_hbm.at[1 - lax.rem(k, 2), k // 2], out_sem.at[k])

    def finish(k):
        d_all(k).wait_recv()
        out_copy(k).start()

    for copy in loads[:4]:
        copy.wait()
    for i in range(3):
        halo_do(i, 1, "start")

    @pl.when(brick == 0)
    def _():
        halo[:, :, 0] = jnp.zeros((2, STEPS, LEVELS, COLS), F32)

    @pl.when(brick == 31)
    def _():
        halo[:, :, 1] = jnp.zeros((2, STEPS, LEVELS, COLS), F32)

    @pl.when(sub == 0)
    def _():
        prior[...] = jnp.zeros(prior.shape, F32)

    for copy in loads[4:]:
        copy.wait()
    for copy in tables:
        copy.wait()

    def each_round(j, carry):
        def within(i):
            return jnp.logical_and(i >= 0, i < CHUNKS)

        def stage(i, work, also=True):
            pl.when(jnp.logical_and(within(i), also))(lambda: work(i))

        def ahead(i):
            halo_do(i, 1, "start")

        def from_prior(k):
            pl.when(sub > 0)(lambda: prior_copy(k - 1).wait_recv())
            start_chunk(k, 0, prior)

        even, odd = lax.rem(j, 2) == 0, lax.rem(j, 2) == 1
        for step in range(STEPS, 0, -1):
            stage(j - step + 1, lambda i, step=step: edge_event(i, step))
        stage(j + 3, ahead)
        stage(j - 3, lambda i: inner_event(i, 4))
        stage(j - 3, lambda i: prior_copy(i).start(), jnp.logical_and(odd, sub < 3))
        stage(j - 4, lambda k: start_chunk(k, 1, two_buf.at[0]), even)
        stage(j - 4, from_prior, odd)
        for step in range(STEPS - 1, 0, -1):
            stage(j - step + 1, lambda i, step=step: inner_event(i, step))
        stage(j - 6, second_hop)
        stage(j - 7, transform)
        stage(j - 8, fourth_hop)
        stage(j - 11, finish)
        return carry

    lax.fori_loop(0, CHUNKS + 11, each_round, 0)

    def drain(k, carry):
        for step in (1, STEPS):
            halo_do(k, step, "wait_send")
        a_all(k).wait_send()
        b_all(k).wait_send()
        c_all(k).wait_send()
        d_all(k).wait_send()
        out_copy(k).wait()
        return carry

    lax.fori_loop(0, CHUNKS, drain, 0)

    @pl.when(sub < 3)
    def _():
        for c in range(4):
            prior_copy(2 * c).wait_send()


def vertical_kernel(h_hbm, v_ref, out_hbm, source, result, in_sem, out_sem):
    units = [(s, r) for s in range(2) for r in range(ROWS)]
    reads = [pltpu.make_async_copy(h_hbm.at[s, :, r, :], source.at[s, r], in_sem.at[s, r]) for s, r in units]
    writes = [pltpu.make_async_copy(result.at[s, r], out_hbm.at[s, :, r, :], out_sem.at[s, r]) for s, r in units]
    for copy in reads:
        copy.start()
    high, low = split(v_ref[...])
    wide = jnp.concatenate([high, low], axis=1)
    for first in range(0, len(units), 4):
        for copy in reads[first : first + 4]:
            copy.wait()
        for s, r in units[first : first + 4]:
            top, rest = split(source[s, r])
            result[s, r] = jnp.dot(
                wide, jnp.concatenate([top, top], axis=0), preferred_element_type=F32
            ) + jnp.dot(high, rest, preferred_element_type=F32)
        for copy in writes[first : first + 4]:
            copy.start()
    for copy in writes:
        copy.wait()


def on_device(increments, courant_x, courant_y, spectrum, vertical):
    row_table, col_table = dct_table(NX), dct_table(COLS)
    tables = [halves(t) for t in (row_table, row_table.T, col_table, col_table.T)]
    hbm = pl.BlockSpec(memory_space=pl.ANY)
    slabs = (2, ROWS, LEVELS, COLS)
    dma = pltpu.SemaphoreType.DMA
    whole = jax.ShapeDtypeStruct((2, LEVELS, ROWS, COLS), F32)
    horizontal = pl.pallas_call(
        kernel,
        out_shape=jax.ShapeDtypeStruct((2, 4, 8, 4, ROWS, COLS), F32),
        in_specs=[hbm] * 8,
        out_specs=hbm,
        scratch_shapes=[
            *[pltpu.VMEM(slabs, F32) for _ in range(5)],
            pltpu.VMEM((2, STEPS, 2, LEVELS, COLS), F32),
            pltpu.VMEM((ROWS, LEVELS, COLS), F32),
            pltpu.VMEM((CHUNKS, 32, ROWS, COLS), F32),
            *[pltpu.VMEM((CHUNKS, 8, 4, ROWS, COLS), F32) for _ in range(4)],
            pltpu.VMEM((NX, COLS), F32),
            *[pltpu.VMEM((2, NX, NX), BF16) for _ in range(2)],
            *[pltpu.VMEM((2, COLS, COLS), BF16) for _ in range(2)],
            dma((48,)),
            dma((5,)),
            *[dma((CHUNKS, STEPS, 2)) for _ in range(2)],
            *[dma((4,)) for _ in range(2)],
            *[dma((CHUNKS,)) for _ in range(9)],
        ],
        compiler_params=pltpu.CompilerParams(
            collective_id=0, has_side_effects=True, vmem_limit_bytes=67_043_328
        ),
    )(increments, courant_x, courant_y, spectrum, *[jnp.asarray(t) for t in tables])
    return pl.pallas_call(
        vertical_kernel,
        out_shape=whole,
        in_specs=[hbm, pl.BlockSpec(memory_space=pltpu.VMEM)],
        out_specs=hbm,
        scratch_shapes=[pltpu.VMEM(slabs, F32)] * 2 + [dma((2, ROWS))] * 2,
        compiler_params=pltpu.CompilerParams(vmem_limit_bytes=67_043_328),
    )(horizontal.reshape(whole.shape), vertical)


def solution(mesh):
    wide = P("sub", None, "brick", None)
    return jax.shard_map(
        on_device, mesh=mesh, in_specs=(wide, wide, wide, P(), P()), out_specs=wide, check_vma=False
    )
```

```python
import jax
import jax.numpy as jnp
import ml_dtypes
import numpy as np
from jax import lax
from jax.experimental import pallas as pl
from jax.experimental.pallas import tpu as pltpu
from jax.sharding import PartitionSpec as P

STEPS = 4
ROWS, LEVELS, COLS, NX = 8, 128, 512, 256
MESH = pl.DeviceIdType.MESH
F32, BF16 = jnp.float32, jnp.bfloat16
CHUNKS, CHUNK = 8, 32
XZ_ORDER = ((1, 0), (0, 1), (1, 1), (0, 3), (1, 3), (0, 2), (1, 2))


def dct_table(count):
    one = np.float32
    freq = np.arange(count, dtype=one)[:, None]
    cells = np.arange(count, dtype=one)[None, :]
    angle = one(np.pi) * (cells + one(0.5)) * freq / one(count)
    table = np.cos(angle.astype(np.float64)).astype(one) * np.sqrt(one(2.0) / one(count))
    table[0] *= np.sqrt(one(0.5))
    return table


def halves(table):
    high = table.astype(ml_dtypes.bfloat16)
    low = (table - high.astype(np.float32)).astype(ml_dtypes.bfloat16)
    return np.stack([high, low])


def split(value):
    high = value.astype(BF16)
    return high, (value - high.astype(F32)).astype(BF16)


def product(a, b):
    def dot(u, v):
        return jnp.dot(u, v, preferred_element_type=F32)

    return dot(a[0], b[0]) + (dot(a[0], b[1]) + dot(a[1], b[0]))


def kernel(
    inc_hbm, cx_hbm, cy_hbm, spec_hbm, rt_hbm, rtt_hbm, ct_hbm, ctt_hbm,
    out_hbm,
    inc, cx, cy, one_buf, two_buf, halo, prior, jumps, mid, planes, mid_back, done,
    spec, rt, rtt, ct, ctt,
    load_sem, table_sem, halo_send, halo_recv, prior_send, prior_recv,
    a_send, a_recv, b_send, b_recv, c_send, c_recv, d_send, d_recv, out_sem,
):
    sub, brick = lax.axis_index("sub"), lax.axis_index("brick")
    x, z, y = brick // 16, lax.rem(brick // 4, 4), lax.rem(brick, 4)
    mine = x * 4 + z
    up, down = lax.rem(brick + 1, 32), lax.rem(brick + 31, 32)

    def xz_peer(dx, dz):
        px, pz = lax.rem(x + dx, 2), lax.rem(z + dz, 4)
        return px * 4 + pz, {"brick": px * 16 + pz * 4 + y}

    def y_peer(dy):
        py = lax.rem(y + dy, 4)
        return py, {"brick": brick - y + py}

    def remote(src, dst, send, recv, device):
        return pltpu.make_async_remote_copy(
            src_ref=src, dst_ref=dst, send_sem=send, recv_sem=recv, device_id=device, device_id_type=MESH
        )

    loads = []

    def load(src, dst, s, rows):
        for r in rows:
            copy = pltpu.make_async_copy(src.at[s, :, r, :], dst.at[s, r], load_sem.at[len(loads)])
            copy.start()
            loads.append(copy)

    edges, inner = (0, 7), tuple(range(1, 7))
    for s in (1, 0):
        load(inc_hbm, inc, s, edges)
    for s in (1, 0):
        load(inc_hbm, inc, s, inner)
        load(cx_hbm, cx, s, edges + inner)
        load(cy_hbm, cy, s, edges + inner)
    tables = [
        pltpu.make_async_copy(src, dst, table_sem.at[i])
        for i, (src, dst) in enumerate(
            ((spec_hbm, spec), (rt_hbm, rt), (rtt_hbm, rtt), (ct_hbm, ct), (ctt_hbm, ctt))
        )
    ]
    for copy in tables:
        copy.start()

    barrier = pltpu.get_barrier_semaphore()
    peers = [{"brick": up}, {"brick": down}, {"sub": lax.rem(sub + 1, 4)}, {"sub": lax.rem(sub + 3, 4)}]
    peers += [xz_peer(dx, dz)[1] for dx, dz in XZ_ORDER] + [y_peer(dy)[1] for dy in (1, 2, 3)]
    for peer in peers:
        pl.semaphore_signal(barrier, inc=1, device_id=peer, device_id_type=MESH)

    pl.semaphore_wait(barrier, len(peers))

    def state(step):
        return inc if step == 0 else (one_buf if step % 2 else two_buf)

    def place(i):
        return 1 - lax.rem(i, 2), pl.multiple_of((i // 2) * CHUNK, CHUNK)

    def halo_copies(i, step):
        s, low = place(i)
        t, src, levels = step - 1, state(step - 1), pl.ds(low, CHUNK)
        return (
            remote(src.at[s, 7, levels], halo.at[s, t, 0, levels], halo_send.at[i, t, 0], halo_recv.at[i, t, 0], {"brick": up}),
            remote(src.at[s, 0, levels], halo.at[s, t, 1, levels], halo_send.at[i, t, 1], halo_recv.at[i, t, 1], {"brick": down}),
        )

    def halo_do(i, step, verb):
        live = jnp.logical_or(sub < 3, lax.rem(i, 2) == 1)
        upward, downward = halo_copies(i, step)
        below, above = (upward, downward) if verb == "wait_recv" else (downward, upward)
        pl.when(jnp.logical_and(live, brick > 0))(lambda: getattr(below, verb)())
        pl.when(jnp.logical_and(live, brick < 31))(lambda: getattr(above, verb)())

    def rows(i, step, which, block):
        s, low = place(i)
        src, dst = state(step - 1), state(step)
        lane = lax.broadcasted_iota(jnp.int32, (block, COLS), 1)

        def body(n, carry):
            at = pl.ds(pl.multiple_of(low + n * block, 8), block)
            for r in which:
                center = src[s, r, at]
                north = src[s, r + 1, at] if r < 7 else halo[s, step - 1, 1, at]
                south = src[s, r - 1, at] if r > 0 else halo[s, step - 1, 0, at]
                east = jnp.where(lane == COLS - 1, 0.0, pltpu.roll(center, COLS - 1, 1))
                west = jnp.where(lane == 0, 0.0, pltpu.roll(center, 1, 1))
                flow = cx[s, r, at] * (north - south) + cy[s, r, at] * (east - west)
                spread = (north + south) + (east + west) - 4.0 * center
                dst[s, r, at] = center - 0.5 * flow + 0.2 * spread
            return carry

        lax.fori_loop(0, CHUNK // block, body, 0)

    def edge_event(i, step):
        halo_do(i, step, "wait_recv")
        if step >= 3:
            halo_do(i, step - 1, "wait_send")
        rows(i, step, edges, 16)
        if step < STEPS:
            halo_do(i, step + 1, "start")

    def inner_event(i, step):
        rows(i, step, inner, 8)

    def prior_copy(i):
        levels = pl.ds(place(i)[1], CHUNK)
        return remote(
            two_buf.at[1, :, levels], prior.at[:, levels], prior_send.at[i // 2], prior_recv.at[i // 2],
            {"sub": lax.rem(sub + 1, 4)},
        )

    def start_chunk(k, s, ends):
        levels = pl.ds(place(k)[1], CHUNK)
        for r in range(ROWS):
            jumps[k, :, r, :] = inc[s, r, levels] - ends[r, levels]
        for dx, dz in XZ_ORDER:
            there, device = xz_peer(dx, dz)
            remote(jumps.at[k, pl.ds(there * 4, 4)], mid.at[k, mine], a_send.at[k], a_recv.at[k], device).start()

    def a_all(k):
        part = mid.at[k, pl.ds(0, 7)]
        return remote(part, part, a_send.at[k], a_recv.at[k], {"brick": up})

    def b_all(k):
        return remote(planes.at[k, pl.ds(0, 6)], planes.at[k, pl.ds(0, 6)], b_send.at[k], b_recv.at[k], {"brick": up})

    def c_all(k):
        return remote(mid_back.at[k, pl.ds(0, 6)], mid_back.at[k, pl.ds(0, 6)], c_send.at[k], c_recv.at[k], {"brick": up})

    def d_all(k):
        return remote(done.at[k, pl.ds(0, 28)], done.at[k, pl.ds(0, 28)], d_send.at[k], d_recv.at[k], {"brick": up})

    def second_hop(k):
        a_all(k).wait_recv()
        mid[k, mine] = jumps[k, pl.ds(mine * 4, 4)]
        for dy in (1, 3, 2):
            there, device = y_peer(dy)
            remote(mid.at[k, :, there], planes.at[k, :, y], b_send.at[k], b_recv.at[k], device).start()
        planes[k, :, y] = mid[k, :, y]

    def transform(k):
        b_all(k).wait_recv()
        plane = planes[k].reshape(NX, COLS)
        value = product((rt[0], rt[1]), split(plane))
        value = product(split(value), (ctt[0], ctt[1])) * spec[...]
        value = product(split(value), (ct[0], ct[1]))
        value = product((rtt[0], rtt[1]), split(value))
        planes[k] = value.reshape(8, 4, ROWS, COLS)
        for dy in (1, 3, 2):
            there, device = y_peer(dy)
            remote(planes.at[k, :, there], mid_back.at[k, :, y], c_send.at[k], c_recv.at[k], device).start()
        mid_back[k, :, y] = planes[k, :, y]

    def fourth_hop(k):
        c_all(k).wait_recv()
        for dx, dz in XZ_ORDER:
            there, device = xz_peer(dx, dz)
            remote(mid_back.at[k, there], done.at[k, pl.ds(mine * 4, 4)], d_send.at[k], d_recv.at[k], device).start()
        done[k, pl.ds(mine * 4, 4)] = mid_back[k, mine]

    def out_copy(k):
        return pltpu.make_async_copy(
            done.at[k], out_hbm.at[1 - lax.rem(k, 2), pl.ds((k // 2) * CHUNK, CHUNK)], out_sem.at[k]
        )

    def finish(k):
        d_all(k).wait_recv()
        out_copy(k).start()

    for copy in loads[:4]:
        copy.wait()
    for i in range(3):
        halo_do(i, 1, "start")

    @pl.when(brick == 0)
    def _():
        halo[:, :, 0] = jnp.zeros((2, STEPS, LEVELS, COLS), F32)

    @pl.when(brick == 31)
    def _():
        halo[:, :, 1] = jnp.zeros((2, STEPS, LEVELS, COLS), F32)

    @pl.when(sub == 0)
    def _():
        prior[...] = jnp.zeros(prior.shape, F32)

    for copy in loads[4:]:
        copy.wait()
    for copy in tables:
        copy.wait()

    def each_round(j, carry):
        def within(i):
            return jnp.logical_and(i >= 0, i < CHUNKS)

        def stage(i, work, also=True):
            pl.when(jnp.logical_and(within(i), also))(lambda: work(i))

        def ahead(i):
            halo_do(i, 1, "start")

        def from_prior(k):
            pl.when(sub > 0)(lambda: prior_copy(k - 1).wait_recv())
            start_chunk(k, 0, prior)

        even, odd = lax.rem(j, 2) == 0, lax.rem(j, 2) == 1
        for step in range(STEPS, 0, -1):
            stage(j - step + 1, lambda i, step=step: edge_event(i, step))
        stage(j + 3, ahead)
        stage(j - 3, lambda i: inner_event(i, 4))
        stage(j - 3, lambda i: prior_copy(i).start(), jnp.logical_and(odd, sub < 3))
        stage(j - 4, lambda k: start_chunk(k, 1, two_buf.at[0]), even)
        stage(j - 4, from_prior, odd)
        for step in range(STEPS - 1, 0, -1):
            stage(j - step + 1, lambda i, step=step: inner_event(i, step))
        stage(j - 6, second_hop)
        stage(j - 7, transform)
        stage(j - 8, fourth_hop)
        stage(j - 11, finish)
        return carry

    lax.fori_loop(0, CHUNKS + 11, each_round, 0)

    def drain(k, carry):
        for step in (1, STEPS):
            halo_do(k, step, "wait_send")
        a_all(k).wait_send()
        b_all(k).wait_send()
        c_all(k).wait_send()
        d_all(k).wait_send()
        out_copy(k).wait()
        return carry

    lax.fori_loop(0, CHUNKS, drain, 0)

    @pl.when(sub < 3)
    def _():
        for c in range(4):
            prior_copy(2 * c).wait_send()


def vertical_kernel(h_hbm, v_ref, out_hbm, source, result, in_sem, out_sem):
    units = [(s, r) for s in range(2) for r in range(ROWS)]
    reads = [pltpu.make_async_copy(h_hbm.at[s, :, r, :], source.at[s, r], in_sem.at[s, r]) for s, r in units]
    writes = [pltpu.make_async_copy(result.at[s, r], out_hbm.at[s, :, r, :], out_sem.at[s, r]) for s, r in units]
    for copy in reads:
        copy.start()
    high, low = split(v_ref[...])
    wide = jnp.concatenate([high, low], axis=1)
    for first in range(0, len(units), 4):
        for copy in reads[first : first + 4]:
            copy.wait()
        for s, r in units[first : first + 4]:
            top, rest = split(source[s, r])
            result[s, r] = jnp.dot(
                wide, jnp.concatenate([top, top], axis=0), preferred_element_type=F32
            ) + jnp.dot(high, rest, preferred_element_type=F32)
        for copy in writes[first : first + 4]:
            copy.start()
    for copy in writes:
        copy.wait()


def on_device(increments, courant_x, courant_y, spectrum, vertical):
    row_table, col_table = dct_table(NX), dct_table(COLS)
    tables = [halves(t) for t in (row_table, row_table.T, col_table, col_table.T)]
    hbm = pl.BlockSpec(memory_space=pl.ANY)
    slabs = (2, ROWS, LEVELS, COLS)
    dma = pltpu.SemaphoreType.DMA
    whole = jax.ShapeDtypeStruct((2, LEVELS, ROWS, COLS), F32)
    horizontal = pl.pallas_call(
        kernel,
        out_shape=whole,
        in_specs=[hbm] * 8,
        out_specs=hbm,
        scratch_shapes=[
            *[pltpu.VMEM(slabs, F32) for _ in range(5)],
            pltpu.VMEM((2, STEPS, 2, LEVELS, COLS), F32),
            pltpu.VMEM((ROWS, LEVELS, COLS), F32),
            pltpu.VMEM((CHUNKS, 32, ROWS, COLS), F32),
            *[pltpu.VMEM((CHUNKS, 8, 4, ROWS, COLS), F32) for _ in range(3)],
            pltpu.VMEM((CHUNKS, 32, ROWS, COLS), F32),
            pltpu.VMEM((NX, COLS), F32),
            *[pltpu.VMEM((2, NX, NX), BF16) for _ in range(2)],
            *[pltpu.VMEM((2, COLS, COLS), BF16) for _ in range(2)],
            dma((48,)),
            dma((5,)),
            *[dma((CHUNKS, STEPS, 2)) for _ in range(2)],
            *[dma((4,)) for _ in range(2)],
            *[dma((CHUNKS,)) for _ in range(9)],
        ],
        compiler_params=pltpu.CompilerParams(
            collective_id=0, has_side_effects=True, vmem_limit_bytes=67_043_328
        ),
    )(increments, courant_x, courant_y, spectrum, *[jnp.asarray(t) for t in tables])
    return pl.pallas_call(
        vertical_kernel,
        out_shape=whole,
        in_specs=[hbm, pl.BlockSpec(memory_space=pltpu.VMEM)],
        out_specs=hbm,
        scratch_shapes=[pltpu.VMEM(slabs, F32)] * 2 + [dma((2, ROWS))] * 2,
        compiler_params=pltpu.CompilerParams(vmem_limit_bytes=67_043_328),
    )(horizontal, vertical)


def solution(mesh):
    wide = P("sub", None, "brick", None)
    return jax.shard_map(
        on_device, mesh=mesh, in_specs=(wide, wide, wide, P(), P()), out_specs=wide, check_vma=False
    )
```

```python
import jax
import jax.numpy as jnp
import ml_dtypes
import numpy as np
from jax import lax
from jax.experimental import pallas as pl
from jax.experimental.pallas import tpu as pltpu
from jax.sharding import PartitionSpec as P

STEPS = 4
ROWS, LEVELS, COLS, NX = 8, 128, 512, 256
MESH = pl.DeviceIdType.MESH
F32, BF16 = jnp.float32, jnp.bfloat16
CHUNKS, CHUNK = 8, 32
XZ_ORDER = ((1, 0), (0, 1), (1, 1), (0, 3), (1, 3), (0, 2), (1, 2))


def dct_table(count):
    one = np.float32
    freq = np.arange(count, dtype=one)[:, None]
    cells = np.arange(count, dtype=one)[None, :]
    angle = one(np.pi) * (cells + one(0.5)) * freq / one(count)
    table = np.cos(angle.astype(np.float64)).astype(one) * np.sqrt(one(2.0) / one(count))
    table[0] *= np.sqrt(one(0.5))
    return table


def halves(table):
    high = table.astype(ml_dtypes.bfloat16)
    low = (table - high.astype(np.float32)).astype(ml_dtypes.bfloat16)
    return np.stack([high, low])


def split(value):
    high = value.astype(BF16)
    return high, (value - high.astype(F32)).astype(BF16)


def product(a, b):
    def dot(u, v):
        return jnp.dot(u, v, preferred_element_type=F32)

    return dot(a[0], b[0]) + (dot(a[0], b[1]) + dot(a[1], b[0]))


def kernel(
    inc_hbm, cx_hbm, cy_hbm, spec_hbm, rt_hbm, rtt_hbm, ct_hbm, ctt_hbm,
    out_hbm,
    inc, cx, cy, one_buf, two_buf, halo, prior, jumps, mid, planes, mid_back, done,
    spec, rt, rtt, ct, ctt,
    load_sem, table_sem, halo_send, halo_recv, prior_send, prior_recv,
    a_send, a_recv, b_send, b_recv, c_send, c_recv, d_send, d_recv, out_sem,
):
    sub, brick = lax.axis_index("sub"), lax.axis_index("brick")
    x, z, y = brick // 16, lax.rem(brick // 4, 4), lax.rem(brick, 4)
    mine = x * 4 + z
    up, down = lax.rem(brick + 1, 32), lax.rem(brick + 31, 32)

    def xz_peer(dx, dz):
        px, pz = lax.rem(x + dx, 2), lax.rem(z + dz, 4)
        return px * 4 + pz, {"brick": px * 16 + pz * 4 + y}

    def y_peer(dy):
        py = lax.rem(y + dy, 4)
        return py, {"brick": brick - y + py}

    def remote(src, dst, send, recv, device):
        return pltpu.make_async_remote_copy(
            src_ref=src, dst_ref=dst, send_sem=send, recv_sem=recv, device_id=device, device_id_type=MESH
        )

    loads = []

    def load(src, dst, s, rows):
        for r in rows:
            copy = pltpu.make_async_copy(src.at[s, :, r, :], dst.at[s, r], load_sem.at[len(loads)])
            copy.start()
            loads.append(copy)

    edges, inner = (0, 7), tuple(range(1, 7))
    for s in (1, 0):
        load(inc_hbm, inc, s, edges)
    for s in (1, 0):
        load(inc_hbm, inc, s, inner)
        load(cx_hbm, cx, s, edges + inner)
        load(cy_hbm, cy, s, edges + inner)
    tables = [
        pltpu.make_async_copy(src, dst, table_sem.at[i])
        for i, (src, dst) in enumerate(
            ((spec_hbm, spec), (rt_hbm, rt), (rtt_hbm, rtt), (ct_hbm, ct), (ctt_hbm, ctt))
        )
    ]
    for copy in tables:
        copy.start()

    barrier = pltpu.get_barrier_semaphore()
    peers = [{"brick": up}, {"brick": down}, {"sub": lax.rem(sub + 1, 4)}, {"sub": lax.rem(sub + 3, 4)}]
    peers += [xz_peer(dx, dz)[1] for dx, dz in XZ_ORDER] + [y_peer(dy)[1] for dy in (1, 2, 3)]
    for peer in peers:
        pl.semaphore_signal(barrier, inc=1, device_id=peer, device_id_type=MESH)

    pl.semaphore_wait(barrier, len(peers))

    def state(step):
        return inc if step == 0 else (one_buf if step % 2 else two_buf)

    def place(i):
        return 1 - lax.rem(i, 2), pl.multiple_of((i // 2) * CHUNK, CHUNK)

    def halo_copies(i, step):
        s, low = place(i)
        t, src, levels = step - 1, state(step - 1), pl.ds(low, CHUNK)
        return (
            remote(src.at[s, 7, levels], halo.at[s, t, 0, levels], halo_send.at[i, t, 0], halo_recv.at[i, t, 0], {"brick": up}),
            remote(src.at[s, 0, levels], halo.at[s, t, 1, levels], halo_send.at[i, t, 1], halo_recv.at[i, t, 1], {"brick": down}),
        )

    def halo_do(i, step, verb):
        live = jnp.logical_or(sub < 3, lax.rem(i, 2) == 1)
        upward, downward = halo_copies(i, step)
        below, above = (upward, downward) if verb == "wait_recv" else (downward, upward)
        pl.when(jnp.logical_and(live, brick > 0))(lambda: getattr(below, verb)())
        pl.when(jnp.logical_and(live, brick < 31))(lambda: getattr(above, verb)())

    def rows(i, step, which, block):
        s, low = place(i)
        src, dst = state(step - 1), state(step)
        lane = lax.broadcasted_iota(jnp.int32, (block, COLS), 1)

        def body(n, carry):
            at = pl.ds(pl.multiple_of(low + n * block, 8), block)
            for r in which:
                center = src[s, r, at]
                north = src[s, r + 1, at] if r < 7 else halo[s, step - 1, 1, at]
                south = src[s, r - 1, at] if r > 0 else halo[s, step - 1, 0, at]
                east = jnp.where(lane == COLS - 1, 0.0, pltpu.roll(center, COLS - 1, 1))
                west = jnp.where(lane == 0, 0.0, pltpu.roll(center, 1, 1))
                flow = cx[s, r, at] * (north - south) + cy[s, r, at] * (east - west)
                spread = (north + south) + (east + west) - 4.0 * center
                dst[s, r, at] = center - 0.5 * flow + 0.2 * spread
            return carry

        lax.fori_loop(0, CHUNK // block, body, 0)

    def edge_event(i, step):
        halo_do(i, step, "wait_recv")
        if step >= 3:
            halo_do(i, step - 1, "wait_send")
        rows(i, step, edges, 16)
        if step < STEPS:
            halo_do(i, step + 1, "start")

    def inner_event(i, step):
        rows(i, step, inner, 8)

    def prior_copy(i):
        levels = pl.ds(place(i)[1], CHUNK)
        return remote(
            two_buf.at[1, :, levels], prior.at[:, levels], prior_send.at[i // 2], prior_recv.at[i // 2],
            {"sub": lax.rem(sub + 1, 4)},
        )

    def start_chunk(k, s, ends):
        levels = pl.ds(place(k)[1], CHUNK)
        for r in range(ROWS):
            jumps[k, :, r, :] = inc[s, r, levels] - ends[r, levels]
        for dx, dz in XZ_ORDER:
            there, device = xz_peer(dx, dz)
            remote(jumps.at[k, pl.ds(there * 4, 4)], mid.at[k, mine], a_send.at[k], a_recv.at[k], device).start()

    def a_all(k):
        part = mid.at[k, pl.ds(0, 7)]
        return remote(part, part, a_send.at[k], a_recv.at[k], {"brick": up})

    def b_all(k):
        return remote(planes.at[k, pl.ds(0, 6)], planes.at[k, pl.ds(0, 6)], b_send.at[k], b_recv.at[k], {"brick": up})

    def c_all(k):
        return remote(mid_back.at[k, pl.ds(0, 6)], mid_back.at[k, pl.ds(0, 6)], c_send.at[k], c_recv.at[k], {"brick": up})

    def d_all(k):
        return remote(done.at[k, pl.ds(0, 28)], done.at[k, pl.ds(0, 28)], d_send.at[k], d_recv.at[k], {"brick": up})

    def second_hop(k):
        a_all(k).wait_recv()
        mid[k, mine] = jumps[k, pl.ds(mine * 4, 4)]
        for dy in (1, 3, 2):
            there, device = y_peer(dy)
            remote(mid.at[k, :, there], planes.at[k, :, y], b_send.at[k], b_recv.at[k], device).start()
        planes[k, :, y] = mid[k, :, y]

    def transform(k):
        b_all(k).wait_recv()
        plane = planes[k].reshape(NX, COLS)
        value = product((rt[0], rt[1]), split(plane))
        value = product(split(value), (ctt[0], ctt[1])) * spec[...]
        value = product(split(value), (ct[0], ct[1]))
        value = product((rtt[0], rtt[1]), split(value))
        planes[k] = value.reshape(8, 4, ROWS, COLS)
        for dy in (1, 3, 2):
            there, device = y_peer(dy)
            remote(planes.at[k, :, there], mid_back.at[k, :, y], c_send.at[k], c_recv.at[k], device).start()
        mid_back[k, :, y] = planes[k, :, y]

    def fourth_hop(k):
        c_all(k).wait_recv()
        for dx, dz in XZ_ORDER:
            there, device = xz_peer(dx, dz)
            remote(mid_back.at[k, there], done.at[k, pl.ds(mine * 4, 4)], d_send.at[k], d_recv.at[k], device).start()
        done[k, pl.ds(mine * 4, 4)] = mid_back[k, mine]

    def out_copy(k):
        return pltpu.make_async_copy(
            done.at[k], out_hbm.at[1 - lax.rem(k, 2), pl.ds((k // 2) * CHUNK, CHUNK)], out_sem.at[k]
        )

    def finish(k):
        d_all(k).wait_recv()
        out_copy(k).start()

    for copy in loads[:4]:
        copy.wait()
    for i in range(3):
        halo_do(i, 1, "start")

    @pl.when(brick == 0)
    def _():
        halo[:, :, 0] = jnp.zeros((2, STEPS, LEVELS, COLS), F32)

    @pl.when(brick == 31)
    def _():
        halo[:, :, 1] = jnp.zeros((2, STEPS, LEVELS, COLS), F32)

    @pl.when(sub == 0)
    def _():
        prior[...] = jnp.zeros(prior.shape, F32)

    for copy in loads[4:26]:
        copy.wait()

    def wait_all(copies):
        for copy in copies:
            copy.wait()

    def each_round(j, carry):
        def within(i):
            return jnp.logical_and(i >= 0, i < CHUNKS)

        def stage(i, work, also=True):
            pl.when(jnp.logical_and(within(i), also))(lambda: work(i))

        def ahead(i):
            halo_do(i, 1, "start")

        def from_prior(k):
            pl.when(sub > 0)(lambda: prior_copy(k - 1).wait_recv())
            start_chunk(k, 0, prior)

        even, odd = lax.rem(j, 2) == 0, lax.rem(j, 2) == 1
        pl.when(j == 1)(lambda: wait_all(loads[26:]))
        pl.when(j == 6)(lambda: wait_all(tables))
        for step in range(STEPS, 0, -1):
            stage(j - step + 1, lambda i, step=step: edge_event(i, step))
        stage(j + 3, ahead)
        stage(j - 3, lambda i: inner_event(i, 4))
        stage(j - 3, lambda i: prior_copy(i).start(), jnp.logical_and(odd, sub < 3))
        stage(j - 4, lambda k: start_chunk(k, 1, two_buf.at[0]), even)
        stage(j - 4, from_prior, odd)
        for step in range(STEPS - 1, 0, -1):
            stage(j - step + 1, lambda i, step=step: inner_event(i, step))
        stage(j - 6, second_hop)
        stage(j - 7, transform)
        stage(j - 8, fourth_hop)
        stage(j - 11, finish)
        return carry

    lax.fori_loop(0, CHUNKS + 11, each_round, 0)

    def drain(k, carry):
        for step in (1, STEPS):
            halo_do(k, step, "wait_send")
        a_all(k).wait_send()
        b_all(k).wait_send()
        c_all(k).wait_send()
        d_all(k).wait_send()
        out_copy(k).wait()
        return carry

    lax.fori_loop(0, CHUNKS, drain, 0)

    @pl.when(sub < 3)
    def _():
        for c in range(4):
            prior_copy(2 * c).wait_send()


def vertical_kernel(h_hbm, v_ref, out_hbm, source, result, in_sem, out_sem):
    units = [(s, r) for s in range(2) for r in range(ROWS)]
    reads = [pltpu.make_async_copy(h_hbm.at[s, :, r, :], source.at[s, r], in_sem.at[s, r]) for s, r in units]
    writes = [pltpu.make_async_copy(result.at[s, r], out_hbm.at[s, :, r, :], out_sem.at[s, r]) for s, r in units]
    for copy in reads:
        copy.start()
    high, low = split(v_ref[...])
    wide = jnp.concatenate([high, low], axis=1)
    for first in range(0, len(units), 4):
        for copy in reads[first : first + 4]:
            copy.wait()
        for s, r in units[first : first + 4]:
            top, rest = split(source[s, r])
            result[s, r] = jnp.dot(
                wide, jnp.concatenate([top, top], axis=0), preferred_element_type=F32
            ) + jnp.dot(high, rest, preferred_element_type=F32)
        for copy in writes[first : first + 4]:
            copy.start()
    for copy in writes:
        copy.wait()


def on_device(increments, courant_x, courant_y, spectrum, vertical):
    row_table, col_table = dct_table(NX), dct_table(COLS)
    tables = [halves(t) for t in (row_table, row_table.T, col_table, col_table.T)]
    hbm = pl.BlockSpec(memory_space=pl.ANY)
    slabs = (2, ROWS, LEVELS, COLS)
    dma = pltpu.SemaphoreType.DMA
    whole = jax.ShapeDtypeStruct((2, LEVELS, ROWS, COLS), F32)
    horizontal = pl.pallas_call(
        kernel,
        out_shape=whole,
        in_specs=[hbm] * 8,
        out_specs=hbm,
        scratch_shapes=[
            *[pltpu.VMEM(slabs, F32) for _ in range(5)],
            pltpu.VMEM((2, STEPS, 2, LEVELS, COLS), F32),
            pltpu.VMEM((ROWS, LEVELS, COLS), F32),
            pltpu.VMEM((CHUNKS, 32, ROWS, COLS), F32),
            *[pltpu.VMEM((CHUNKS, 8, 4, ROWS, COLS), F32) for _ in range(3)],
            pltpu.VMEM((CHUNKS, 32, ROWS, COLS), F32),
            pltpu.VMEM((NX, COLS), F32),
            *[pltpu.VMEM((2, NX, NX), BF16) for _ in range(2)],
            *[pltpu.VMEM((2, COLS, COLS), BF16) for _ in range(2)],
            dma((48,)),
            dma((5,)),
            *[dma((CHUNKS, STEPS, 2)) for _ in range(2)],
            *[dma((4,)) for _ in range(2)],
            *[dma((CHUNKS,)) for _ in range(9)],
        ],
        compiler_params=pltpu.CompilerParams(
            collective_id=0, has_side_effects=True, vmem_limit_bytes=67_043_328
        ),
    )(increments, courant_x, courant_y, spectrum, *[jnp.asarray(t) for t in tables])
    return pl.pallas_call(
        vertical_kernel,
        out_shape=whole,
        in_specs=[hbm, pl.BlockSpec(memory_space=pltpu.VMEM)],
        out_specs=hbm,
        scratch_shapes=[pltpu.VMEM(slabs, F32)] * 2 + [dma((2, ROWS))] * 2,
        compiler_params=pltpu.CompilerParams(vmem_limit_bytes=67_043_328),
    )(horizontal, vertical)


def solution(mesh):
    wide = P("sub", None, "brick", None)
    return jax.shard_map(
        on_device, mesh=mesh, in_specs=(wide, wide, wide, P(), P()), out_specs=wide, check_vma=False
    )
```
